32 devices in a mesh: batch: 8 (over y, x, core), slab: 4 (over z).
Axes of the slice: x: 2, y: 2, z: 4, core: 2. Of those that a mesh axis runs over, the one named last changes fastest.
Arguments:
- volumes: float32 [16, 128, 128, 128], P('batch', 'slab'), may hold values from -6 to 6
- tilt_low: int32 [16], P('batch'), may hold values from -70 to -40
- tilt_high: int32 [16], P('batch'), may hold values from 40 to 70
- shifts: int32 [16, 3], P('batch'), may hold values from 0 to 127
- support: float32 [128, 128, 128], P('slab'), may hold values from 0.2 to 1
Outputs:
- average: float32 [128, 128, 128], P('slab')
- misfits: float32 [3], replicated
The draws below stay inside these ranges and needn't reach their ends.
Inputs may be any that keep to these rules, and one draw needn't show every extreme that they name: `shifts`: columns hold the shift along z, y and x.
All inputs are finite; a program needn't handle non-finite values.
Results may differ from the reference program's by a relative error of at most 0.0003.
Values sent between devices are 32-bit elements; how exact they have to be, the bound alone decides.
No kernel may reach another device: no remote copies, remote signals or barrier semaphores. Data moves between devices by JAX's collectives and lax.ppermute only.
A program may use at most 64 MiB of HBM per device.

```python
import math
import jax
import jax.numpy as jnp
from jax import lax

N = 128
ITERS = 3
SUBS = 16


def with_ends(array, rng, smallest, top_value):
    index_at = [jax.random.randint(jax.random.fold_in(rng, axis), (), 0, length) for axis, length in enumerate(array.shape)]
    longest = array.shape.index(max(array.shape))
    next_to = index_at[:longest] + [(index_at[longest] + 1) % array.shape[longest]] + index_at[longest + 1:]
    return array.at[tuple(index_at)].set(smallest).at[tuple(next_to)].set(top_value)


def shard_levels(rng, shape, split, smallest, largest):
    def one(axis_at, shards_of):
        draws = jax.random.uniform(jax.random.fold_in(jax.random.fold_in(rng, 6), axis_at), (shards_of,), jnp.float32, smallest / len(split), largest / len(split))
        return jnp.repeat(jnp.exp(draws), shape[axis_at] // shards_of).reshape((-1,) + (1,) * (len(shape) - axis_at - 1))

    gain = one(*split[0])
    for cut in split[1:]:
        gain = gain * one(*cut)
    return gain


def bell_draw(own_key, extent, deviation, bound, shards=(), kind=jnp.bfloat16):
    loudness = shard_levels(own_key, extent, shards, -0.22, 0.18) if shards else 1.0
    result = jax.random.normal(own_key, extent, jnp.float32) * deviation * loudness
    return jnp.minimum(jnp.maximum(result, -bound), bound).astype(kind)


def setup_inputs(seed: int = 0) -> dict:
    streams_of = jax.random.split(jax.random.key(seed), 6)
    return {
        "volumes": bell_draw(streams_of[0], (SUBS, N, N, N), 1.0, 6.0, ((0, 8), (1, 4)), jnp.float32),
        "tilt_low": with_ends(jax.random.randint(streams_of[1], (SUBS,), -70, -39), jax.random.fold_in(streams_of[1], 1), -70, (-39) - 1).astype(jnp.int32),
        "tilt_high": with_ends(jax.random.randint(streams_of[2], (SUBS,), 40, 71), jax.random.fold_in(streams_of[2], 1), 40, 70).astype(jnp.int32),
        "shifts": with_ends(jax.random.randint(streams_of[3], (SUBS, 3), 0, N), jax.random.fold_in(streams_of[3], 1), 0, N - 1).astype(jnp.int32),
        "support": jnp.clip(0.2 + 0.8 * jax.random.uniform(streams_of[4], (N, N, N), jnp.float32) ** shard_levels(streams_of[4], (N, N, N), ((0, 4),), -0.2, 0.2), 0.2, 1.0),
    }


REG_WEIGHT = 0.5
FLOOR_VALUE = 1.0
SOFTNESS = 5.0
TO_DEGREES = 180.0 / math.pi


def signed(length):
    index = jnp.arange(length, dtype=jnp.int32)
    return jnp.where(index < length // 2, index, index - length)


def wedge(low, high, length):
    depth = signed(length)[:, None]
    across = signed(length)[None, :]
    facing = jnp.where(across >= 0, 1, -1)
    theta = jnp.arctan2((depth * facing).astype(jnp.float32), jnp.abs(across).astype(jnp.float32)) * TO_DEGREES
    lower = low.astype(jnp.float32)
    upper = high.astype(jnp.float32)
    return jax.nn.sigmoid((upper - theta) / SOFTNESS) * jax.nn.sigmoid((theta - lower) / SOFTNESS)


def spectrum(volume, offset):
    index = jnp.arange(N, dtype=jnp.int32)
    values = jnp.fft.fftn(volume, norm="ortho")
    turns = (index[:, None, None] * offset[0] + index[None, :, None] * offset[1] + index[None, None, :] * offset[2]) % N
    angle = turns.astype(jnp.float32) * (2.0 * math.pi / N)
    cosine = jnp.cos(angle)
    sine = jnp.sin(angle)
    return values.real * cosine + values.imag * sine, values.imag * cosine - values.real * sine


def reference(volumes, tilt_low, tilt_high, shifts, support):
    def gather_sums(carry, item):
        volume, low, high, offset = item
        weight = wedge(low, high, N)
        spread = weight[:, None, :]
        shifted_real, shifted_imag = spectrum(volume, offset)
        return (carry[0] + spread * shifted_real, carry[1] + spread * shifted_imag, carry[2] + weight * weight), None

    empty = jnp.zeros((N, N, N), jnp.float32)
    start = (empty, empty, jnp.zeros((N, N), jnp.float32))
    (sum_real, sum_imag, weight_sum), _ = lax.scan(gather_sums, start, (volumes, tilt_low, tilt_high, shifts))
    divisor_base = weight_sum[:, None, :]
    mean_real = empty
    mean_imag = empty
    misfits = []
    average = empty
    for turn in range(ITERS):
        def add_misfit(total, item):
            volume, low, high, offset = item
            spread = wedge(low, high, N)[:, None, :]
            shifted_real, shifted_imag = spectrum(volume, offset)
            diff_real = shifted_real - spread * mean_real
            diff_imag = shifted_imag - spread * mean_imag
            return total + jnp.sum(diff_real * diff_real + diff_imag * diff_imag), None

        total, _ = lax.scan(add_misfit, jnp.zeros((), jnp.float32), (volumes, tilt_low, tilt_high, shifts))
        mean_misfit = total / (SUBS * float(N * N * N))
        misfits.append(mean_misfit)
        damping = REG_WEIGHT * SUBS * mean_misfit + FLOOR_VALUE
        divisor = divisor_base + damping
        new_real = mean_real + (sum_real - divisor_base * mean_real) / divisor
        new_imag = mean_imag + (sum_imag - divisor_base * mean_imag) / divisor
        field = jnp.fft.ifftn(new_real + 1j * new_imag, norm="ortho").real
        average = support * field
        if turn + 1 < ITERS:
            values = jnp.fft.fftn(average, norm="ortho")
            mean_real = values.real
            mean_imag = values.imag
    return average, jnp.stack(misfits)
```

```python
import functools
import math

import jax
import jax.numpy as jnp
import numpy as np
from jax import lax
from jax.experimental import pallas as pl
from jax.experimental.pallas import tpu as pltpu
from jax.sharding import PartitionSpec as P

ITERS = 3

REG_WEIGHT = 0.5
FLOOR_VALUE = 1.0
SOFTNESS = 5.0
HIGHEST = lax.Precision.HIGHEST
BF16 = jnp.bfloat16
F32 = jnp.float32
STREAMS = 2


def np_packed(n):
    half = n // 2
    row = np.arange(n)[:, None]
    lane = np.arange(n)[None, :]
    edge = (lane % half == 0) | (row < 0)
    kx = np.where(edge, lane, lane % half) + 0 * row
    kz = np.where(edge & (row > half), row - half, row + 0 * lane)
    return kz, kx, edge


def np_theta(kz, kx, n):
    signed = lambda k: np.where(k < n // 2, k, k - n)
    across = signed(kx)
    facing = np.where(across >= 0, 1, -1)
    return np.degrees(np.arctan2((signed(kz) * facing).astype(np.float64), np.abs(across))).astype(np.float32)


def np_split(table):
    high = table.astype(BF16)
    low = (table - high.astype(np.float64)).astype(BF16)
    return high, low


def np_x_forward(n):
    half = n // 2
    x = np.arange(n)[:, None]
    lane = np.arange(n)[None, :]
    angle = 2 * np.pi * ((x * (lane % half)) % n) / n
    bulk = lane % half != 0
    real, imag = np.cos(angle) * bulk, -np.sin(angle) * bulk
    left = lane < half
    plain = np.where(left, real, imag)
    turned = np.where(left, imag, -real)
    ends = np.where(lane == 0, 1.0, np.where(lane == half, (-1.0) ** x, 0.0))
    return np.concatenate([plain, turned, ends], axis=1) / math.sqrt(n)


def np_z_forward(n):
    half = n // 2
    k = np.arange(n)[:, None]
    z = np.arange(n)[None, :]
    angle = lambda k: 2 * np.pi * ((k * z) % n) / n
    packed = np.where(k <= half, np.cos(angle(k)), -np.sin(angle(k - half)))
    return np.concatenate([np.cos(angle(k)), np.sin(angle(k)), packed], axis=1) / math.sqrt(n)


def np_x_backward(n):
    half = n // 2
    lane = np.arange(n)[:, None]
    x = np.arange(n)[None, :]
    angle = 2 * np.pi * ((x * (lane % half)) % n) / n
    bulk = 2.0 * (lane % half != 0)
    left = lane < half
    first = np.where(left, np.cos(angle), -np.sin(angle)) * bulk
    second = np.where(left, np.sin(angle), np.cos(angle)) * bulk
    ends = np.where(lane == 0, 1.0, np.where(lane == half, (-1.0) ** x, 0.0))
    return np.concatenate([first, second, ends], axis=1) / math.sqrt(n)


def np_z_backward(n):
    half = n // 2
    z = np.arange(n)[:, None]
    k = np.arange(n)[None, :]
    angle = lambda k: 2 * np.pi * ((k * z) % n) / n
    count = np.where(k % half == 0, 1.0, 2.0)
    packed = count * np.where(k <= half, np.cos(angle(k)), -np.sin(angle(k - half)))
    return np.concatenate([np.cos(angle(k)), -np.sin(angle(k)), packed], axis=1) / math.sqrt(n)


def np_left(table):
    high, low = np_split(table)
    return np.concatenate([high, high, low], axis=1)


def np_right(table):
    high, low = np_split(table)
    return np.concatenate([high, high, low], axis=0)


def split_graph(table):
    high = lax.reduce_precision(table, 8, 7)
    return high.astype(BF16), (table - high).astype(BF16)


def shifted_tables(offset_z, offset_x, start, layer, n):
    half = n // 2
    step = F32(2.0 * math.pi / n)
    scale = F32(1.0 / math.sqrt(n))
    x = jnp.arange(n, dtype=jnp.int32)[None, :, None] + offset_x[:, None, None]
    wide = np.arange(3 * n)
    lane = wide % n
    part = wide // n
    kx = np.where(part < 2, lane % half, lane)
    quarter = np.select([(part == 0) & (lane < half), (part == 0), (part == 1) & (lane < half), part == 1], [0, 1, 1, 2], 0)
    keep = np.where(part < 2, lane % half != 0, lane % half == 0)
    turns = (x * jnp.asarray(kx, jnp.int32) + jnp.asarray(quarter * (n // 4), jnp.int32)) % n
    right = jnp.cos(turns.astype(F32) * step) * jnp.asarray(np.where(keep, 1.0 / math.sqrt(n), 0.0), F32)
    z = jnp.arange(layer, dtype=jnp.int32)[None, None, :] + start + offset_z[:, None, None]
    k = np.arange(n)[:, None]
    rows = [(k, 0), (k, -1), (np.where(k <= half, k, k - half), np.where(k <= half, 0, 1))]
    left = []
    for row, turn in rows:
        turns = (z * jnp.asarray(row, jnp.int32) + jnp.asarray(turn * (n // 4) + 0 * row, jnp.int32)) % n
        left.append(jnp.cos(turns.astype(F32) * step) * scale)
    right_high, right_low = split_graph(right)
    left_high, left_low = split_graph(jnp.concatenate(left, axis=2))
    return (
        jnp.concatenate([right_high, right_high, right_low], axis=1),
        jnp.concatenate([left_high, left_high, left_low], axis=2),
    )


def wedge(low, high, theta):
    lower = low.astype(F32)[:, None, None]
    upper = high.astype(F32)[:, None, None]
    return jax.nn.sigmoid((upper - theta) / SOFTNESS) * jax.nn.sigmoid((theta - lower) / SOFTNESS)


def split_value(value):
    high = value.astype(BF16)
    return high, (value - high.astype(F32)).astype(BF16)


def times_right(value, table):
    high, low = split_value(value)
    n = high.shape[1]
    return jnp.dot(jnp.concatenate([high, low], axis=1), table[: 2 * n], preferred_element_type=F32) + jnp.dot(
        high, table[2 * n :], preferred_element_type=F32
    )


def times_left(table, high, low):
    depth = high.shape[0]
    return jnp.dot(table[:, : 2 * depth], jnp.concatenate([high, low], axis=0), preferred_element_type=F32) + jnp.dot(
        table[:, 2 * depth :], high, preferred_element_type=F32
    )


def stacked(wide, n):
    return jnp.concatenate([wide[:, :n], wide[:, n : 2 * n], wide[:, 2 * n :]], axis=0)


GROUP = 8


def gather_kernel(groups_of, source_ref, right_ref, left_ref, weight_ref, *rest):
    parts = len(groups_of)
    volume_count = source_ref.shape[0]
    holders = rest[: len(rest) - parts - 2]
    outs = rest[len(holders) : len(holders) + parts]
    held, sems = rest[-2:]
    per = holders[0].shape[0]
    layer, n = held.shape[2], held.shape[3]
    planes = sum(groups_of) * GROUP

    def copy(volume, plane):
        return pltpu.make_async_copy(
            holders[volume // per].at[volume % per, :, source_ref[volume, plane], :], held.at[volume, plane], sems.at[volume, plane]
        )

    for plane in range(planes):
        for volume in range(volume_count):
            copy(volume, plane).start()

    base = 0
    for out, groups in zip(outs, groups_of):

        def one(group, carry, out=out, base=base):
            for volume in range(volume_count):
                for inner in range(GROUP):
                    copy(volume, base + group * GROUP + inner).wait()
            for volume in range(volume_count):
                rows = held[volume, pl.ds(base + group * GROUP, GROUP)].reshape(GROUP * layer, n)
                wide = times_right(rows, right_ref[volume])
                high, low = split_value(wide)
                for pair in range(GROUP // 2):
                    both = [slice((2 * pair + i) * layer, (2 * pair + i + 1) * layer) for i in range(2)]
                    spectrum = times_left(
                        left_ref[volume],
                        jnp.concatenate([stacked(high[rows_of], n) for rows_of in both], axis=1),
                        jnp.concatenate([stacked(low[rows_of], n) for rows_of in both], axis=1),
                    )
                    for i in range(2):
                        value = weight_ref[volume] * spectrum[:, i * n : (i + 1) * n]
                        at = group * GROUP + 2 * pair + i
                        out[at] = value if volume == 0 else out[at] + value
            return carry

        lax.fori_loop(0, groups, one, 0)
        base += groups * GROUP


def gather_planes(volumes, sources, right, left, weight, counts):
    volume_count, planes = sources.shape
    per, layer, n, _ = volumes[0].shape
    return pl.pallas_call(
        functools.partial(gather_kernel, tuple(count // GROUP for count in counts)),
        out_shape=[jax.ShapeDtypeStruct((count, n, n), F32) for count in counts],
        in_specs=[pl.BlockSpec(memory_space=pltpu.SMEM)]
        + [pl.BlockSpec(memory_space=pltpu.VMEM)] * 3
        + [pl.BlockSpec(memory_space=pl.ANY)] * len(volumes),
        out_specs=[pl.BlockSpec(memory_space=pltpu.VMEM)] * len(counts),
        scratch_shapes=[
            pltpu.VMEM((volume_count, planes, layer, n), F32),
            pltpu.SemaphoreType.DMA((volume_count, planes)),
        ],
        name="gather_planes",
    )(sources, right, left, weight, *volumes)


def refine_kernel(first, last, weights_of, peers, *refs):
    refs = list(refs)
    take = lambda count: [refs.pop(0) for _ in range(count)]
    (parts_ref, energy_ref, ws_ref, special_ref, ends_ref, mult_ref, support_ref, xb_ref, zb_ref) = take(9)
    if not last:
        xf_ref, zf_ref = take(2)
    if first:
        pieces = take(weights_of)
    else:
        sum_ref, mean_ref = take(2)
    misfit_ref = take(1)[0]
    if last:
        average_ref = take(1)[0]
    else:
        new_mean_ref, part_ref = take(2)
        if first:
            kept_ref = take(1)[0]
    (held_ref,) = take(1)
    n = ws_ref.shape[1]
    planes = ends_ref.shape[0]
    cells, volume_total = energy_ref[1, 0], energy_ref[2, 0]
    total = energy_ref[0:1, :]
    if not first:
        total = total + jnp.sum(parts_ref[...], axis=0, keepdims=True)
    total = jnp.sum(total)
    misfit = total / (volume_total * cells)
    misfit_ref[...] = jnp.full(misfit_ref.shape, misfit, F32)
    damping = REG_WEIGHT * volume_total * misfit + FLOOR_VALUE
    ws = ws_ref[0]
    ws_mirror = ws_ref[1]
    inverse = 1.0 / (ws + damping)
    inverse_mirror = 1.0 / (ws_mirror + damping)
    special = special_ref[...] > 0.5
    sums = []
    uppers = []
    for plane in range(planes):
        if first:
            per = planes // (2 * weights_of)
            color, inner = plane // (planes // 2), plane % (planes // 2)
            piece = pieces[inner // per]
            value = piece[0, color, inner % per]
            for source in range(1, piece.shape[0]):
                value = value + piece[source, color, inner % per]
            if not last:
                kept_ref[plane] = value
        else:
            value = sum_ref[plane]
        mirror = jnp.where(special, ends_ref[plane], value)
        sums.append((value, mirror))
        if first:
            upper = 0.5 * (value * inverse + mirror * inverse_mirror)
        else:
            pulled = damping * mean_ref[plane]
            upper = 0.5 * ((pulled + value) * inverse + (pulled + mirror) * inverse_mirror)
        uppers.append(upper)
    wide = times_right(jnp.concatenate(uppers, axis=0), xb_ref[...])
    high, low = split_value(wide)

    def z_step(table_ref, high, low):
        result = []
        for pair in range((planes + 1) // 2):
            members = [p for p in (2 * pair, 2 * pair + 1) if p < planes]
            field = times_left(
                table_ref[...],
                jnp.concatenate([stacked(high[p * n : (p + 1) * n], n) for p in members], axis=1),
                jnp.concatenate([stacked(low[p * n : (p + 1) * n], n) for p in members], axis=1),
            )
            result += [field[:, i * n : (i + 1) * n] for i in range(len(members))]
        return result

    fields = z_step(zb_ref, high, low)
    layer = support_ref.shape[2]
    averages = []
    for plane in range(planes):
        for slab in range(support_ref.shape[0]):
            piece = support_ref[slab, plane] * fields[plane][slab * layer : (slab + 1) * layer]
            if last:
                average_ref[slab, plane] = piece
            else:
                averages.append(piece)
    if last:
        return
    wide = times_right(jnp.concatenate(averages, axis=0), xf_ref[...])
    high, low = split_value(wide)
    means = z_step(zf_ref, high, low)
    ws_both = 0.5 * (ws + ws_mirror)
    acc = jnp.zeros((n, n), F32)
    for plane in range(planes):
        mean = means[plane]
        value, mirror = sums[plane]
        new_mean_ref[plane] = mean
        acc = acc + mean * (ws_both * mean - (value + mirror))
    acc = jnp.sum(acc * mult_ref[...], axis=0, keepdims=True)
    part_ref[...] = jnp.broadcast_to(acc, part_ref.shape)


def refine(first, last, parts, energy, ws, ends, support, pieces, peers):
    n = ws.shape[1]
    planes = ends.shape[0]
    slabs, _, layer, _ = support.shape
    kz, kx, edge = np_packed(n)
    special = (edge | (kz == n // 2)).astype(np.float32)
    lone = edge & (np.arange(n)[:, None] % (n // 2) == 0)
    mult = np.where(lone, 1.0, 2.0).astype(np.float32)
    args = [parts, energy, ws, special, ends, mult, support, np_right(np_x_backward(n)), np_left(np_z_backward(n))]
    if not last:
        args += [np_right(np_x_forward(n)), np_left(np_z_forward(n))]
    args += list(pieces)
    shape = lambda *dims: jax.ShapeDtypeStruct(dims, F32)
    outs = [shape(1, n)]
    if last:
        outs += [shape(slabs, planes, layer, n)]
    else:
        outs += [shape(planes, n, n), shape(peers, n)]
        if first:
            outs += [shape(planes, n, n)]
    return pl.pallas_call(
        functools.partial(refine_kernel, first, last, len(pieces), peers),
        out_shape=outs,
        in_specs=[pl.BlockSpec(memory_space=pltpu.VMEM)] + [pl.BlockSpec(memory_space=pltpu.SMEM) if False else pl.BlockSpec(memory_space=pltpu.VMEM)] * (len(args) - 1),
        out_specs=[pl.BlockSpec(memory_space=pltpu.VMEM)] * len(outs),
        scratch_shapes=[pltpu.VMEM((8, n), F32)],
        name="refine",
    )(*[jnp.asarray(arg) for arg in args])


def extras(volumes, info, start, order, n):
    half = n // 2
    layer = volumes.shape[1]
    kz, kx, _ = np_packed(n)
    theta = np_theta((n - kz) % n, (n - kx) % n, n)
    mirrored = wedge(info[:, 0], info[:, 1], jnp.asarray(theta))
    sign = lambda index: (1 - 2 * (index % 2)).astype(F32)
    x_sign = sign(jnp.arange(n, dtype=jnp.int32)[None, :] + info[:, 4:5])
    z_sign = sign(jnp.arange(layer, dtype=jnp.int32)[None, :] + start + info[:, 2:3])
    ends = jnp.stack([jnp.sum(volumes, axis=3), jnp.sum(volumes * x_sign[:, None, None, :], axis=3)], axis=1)
    middle = jnp.sum(volumes * z_sign[:, :, None, None], axis=1)
    z = jnp.arange(layer, dtype=jnp.int32)[None, None, :] + start + info[:, 2][:, None, None]
    k = np.arange(n)[:, None]
    row = np.where(k <= half, k, k - half)
    turns = (z * jnp.asarray(row, jnp.int32) + jnp.asarray(np.where(k <= half, 0, n // 4), jnp.int32)) % n
    z_table = jnp.cos(turns.astype(F32) * F32(2.0 * math.pi / n)) * F32(1.0 / n)
    columns = jnp.einsum("skz,sczy->syck", z_table, ends, precision=HIGHEST)
    columns = columns * jnp.stack([mirrored[:, :, 0], mirrored[:, :, half]], axis=1)[:, None]
    lane = np.arange(n)
    x = jnp.arange(n, dtype=jnp.int32)[None, :, None] + info[:, 4][:, None, None]
    turns = (x * jnp.asarray(lane % half, jnp.int32) + jnp.asarray(np.where(lane < half, 0, n // 4), jnp.int32)) % n
    x_table = jnp.cos(turns.astype(F32) * F32(2.0 * math.pi / n)) * F32(1.0 / n)
    across = jnp.einsum("syx,sxc->syc", middle, x_table, precision=HIGHEST) * mirrored[:, half, None, :]
    rows = jnp.concatenate([columns, across[:, :, None, :]], axis=2)
    place = (jnp.asarray(order, jnp.int32)[None, :] - info[:, 3:4]) % n
    chosen = (place[:, :, None] == jnp.arange(n, dtype=jnp.int32)).astype(F32)
    return jnp.einsum("spy,syck->pck", chosen, rows, precision=HIGHEST)


def end_planes(rows, n):
    half = n // 2
    lane = jnp.arange(n)[None, None, :]
    row = jnp.arange(n)[None, :, None]
    value = jnp.where((row == half), rows[:, 2, None, :], 0.0)
    value = jnp.where(lane == 0, rows[:, 0, :, None], value)
    return jnp.where(lane == half, rows[:, 1, :, None], value)


def squares(low, high, n):
    kz, kx, _ = np_packed(n)
    result = []
    for theta in (np_theta(kz, kx, n), np_theta((n - kz) % n, (n - kx) % n, n)):
        weight = wedge(low, high, jnp.asarray(theta))
        result.append(jnp.sum(weight * weight, axis=0))
    return jnp.stack(result)


def body(volumes, tilt_low, tilt_high, shifts, support):
    items, layer, n = volumes.shape[0], volumes.shape[1], volumes.shape[3]
    batches, slabs = lax.axis_size("batch"), lax.axis_size("slab")
    place, slab = lax.axis_index("batch"), lax.axis_index("slab")
    start = slab * layer
    subs = items * batches
    info = jnp.concatenate([tilt_low[:, None], tilt_high[:, None], shifts], axis=1)
    kz, kx, _ = np_packed(n)
    theta = jnp.asarray(np_theta(kz, kx, n))
    spread = batches == 8 and n % (8 * slabs * 2 * STREAMS) == 0
    swap = lambda value, bit: lax.ppermute(value, "batch", [(i, i ^ bit) for i in range(batches)])
    own_energy = jnp.sum(volumes * volumes)
    lanes = jnp.arange(n, dtype=jnp.int32)
    mine = lambda row: jnp.sum(
        jnp.where(lanes[None, :] == (place * items + jnp.arange(items, dtype=jnp.int32))[:, None], row.astype(F32)[:, None], 0.0), axis=0
    )

    if not spread:
        order = np.arange(n)
        right, left = shifted_tables(info[:, 2], info[:, 4], start, layer, n)
        weight = wedge(info[:, 0], info[:, 1], theta)
        source = (lanes[None, :] - info[:, 3:4]) % n
        (sums,) = gather_planes([volumes], source, right, left, weight, [n])
        sums = lax.psum_scatter(lax.psum(sums, "batch"), "slab", scatter_dimension=0, tiled=True)
        rows = extras(volumes, info, start, order, n)
        facts = jnp.stack([mine(info[:, 0]), mine(info[:, 1]), jnp.full((n,), own_energy)])
        rows, facts = lax.psum((rows, facts), ("batch", "slab"))
        planes = n // slabs
        rows = lax.dynamic_slice_in_dim(rows, slab * planes, planes, axis=0)
        pieces = [sums.reshape(1, 2, planes // 2, n, n)]
        support_planes = lax.all_to_all(support.transpose(1, 0, 2), "slab", split_axis=0, concat_axis=0, tiled=True)
        support_planes = support_planes.reshape(slabs, planes, layer, n)
        peers = 1
        share = lambda value: lax.psum(value, "slab")
    else:
        partner = swap(volumes, 1)
        partner_info = swap(info, 1)
        both = jnp.concatenate([info, partner_info], axis=0)
        right, left = shifted_tables(both[:, 2], both[:, 4], start, layer, n)
        weight = wedge(both[:, 0], both[:, 1], theta)
        core, at_x, at_y = place % 2, (place // 2) % 2, place // 4
        inner = n // (16 * slabs)
        per = inner // STREAMS

        def plane_of(core, color, at_y, at_x, at_z, at_j):
            return ((((core * 2 + color) * 2 + at_y) * 2 + at_x) * slabs + at_z) * inner + at_j

        at_z = np.arange(slabs)[:, None]
        sent, kept = [], []
        for stream in range(STREAMS):
            at_j = np.arange(per)[None, :] + stream * per
            for held, flip in ((sent, True), (kept, False)):
                targets = []
                near_x, near_y = (1 - at_x, 1 - at_y) if flip else (at_x, at_y)
                targets += [plane_of(core, 0, y, near_x, at_z, at_j).reshape(-1) for y in (1 - at_y, at_y)]
                targets += [plane_of(core, 1, near_y, x, at_z, at_j).reshape(-1) for x in (1 - at_x, at_x)]
                source = (jnp.concatenate(targets)[None, :] - both[:, 3:4]) % n
                count = 2 * slabs * per
                held.append(gather_planes([volumes, partner], source.astype(jnp.int32), right, left, weight, [count, count]))
        pieces = []
        for stream in range(STREAMS):
            halves = []
            for color, (near, far) in enumerate(((2, 4), (4, 2))):
                got = swap(sent[stream][color], near).reshape(2, slabs, per, n, n)
                own = kept[stream][color].reshape(2, slabs, per, n, n)
                second = swap(got[0] + own[0], far)
                halves.append(second + (got[1] + own[1]))
            pieces.append(lax.all_to_all(jnp.stack(halves, axis=1), "slab", split_axis=0, concat_axis=0, tiled=True))
        planes = 2 * inner
        index = np.arange(batches)
        order = plane_of(
            (index % 2)[:, None, None, None],
            np.arange(2)[None, None, :, None],
            (index // 4)[:, None, None, None],
            ((index // 2) % 2)[:, None, None, None],
            np.arange(slabs)[None, :, None, None],
            np.arange(inner)[None, None, None, :],
        ).reshape(-1)
        peers = batches * slabs
        rows = extras(volumes, info, start, order, n).reshape(peers, planes * 3, n)
        facts = jnp.stack([mine(info[:, 0]), mine(info[:, 1]), jnp.full((n,), own_energy)])
        packed = jnp.concatenate([rows, jnp.broadcast_to(facts[None], (peers, 3, n)), jnp.zeros((peers, -(planes * 3 + 3) % 8, n), F32)], axis=1)
        packed = lax.all_to_all(packed, ("batch", "slab"), split_axis=0, concat_axis=0, tiled=True)
        packed = jnp.sum(packed, axis=0)
        rows, facts = packed[: planes * 3].reshape(planes, 3, n), packed[planes * 3 : planes * 3 + 3]
        viewed = support.reshape(layer, 2, 2, 4, slabs, inner, n)
        viewed = lax.dynamic_slice(viewed, (0, core, 0, at_y * 2 + at_x, 0, 0, 0), (layer, 1, 2, 1, slabs, inner, n))
        viewed = viewed.reshape(layer, 2, slabs, inner, n).transpose(2, 1, 3, 0, 4).reshape(slabs, planes, layer, n)
        support_planes = lax.all_to_all(viewed, "slab", split_axis=0, concat_axis=0, tiled=True)
        share = lambda value: lax.all_to_all(value, ("batch", "slab"), split_axis=0, concat_axis=0, tiled=True)

    low = facts[0, :subs] / slabs
    high = facts[1, :subs] / slabs
    ws = squares(low, high, n)
    lane0 = (lanes == 0)[None, :]
    energy = jnp.concatenate(
        [jnp.where(lane0, facts[2:3], 0.0), jnp.full((1, n), float(n) ** 3, F32), jnp.full((1, n), float(subs), F32)], axis=0
    )
    ends = end_planes(rows, n)
    misfits = []
    parts = jnp.zeros((peers, n), F32)
    for turn in range(ITERS):
        first, last = turn == 0, turn + 1 == ITERS
        result = refine(first, last, parts, energy, ws, ends, support_planes, pieces, peers)
        misfits.append(result[0][0, 0])
        if last:
            average = result[1]
        else:
            if first:
                sums = result[3]
            pieces = (sums, result[1])
            parts = share(result[2])
    misfits = jnp.stack(misfits)

    average = lax.all_to_all(average, "slab", split_axis=0, concat_axis=0, tiled=True)
    if not spread:
        return average.transpose(2, 0, 1, 3).reshape(layer, n, n), misfits
    average = average.reshape(slabs, 2, inner, layer, n)
    blocks = []
    for color, (near, far) in enumerate(((2, 4), (4, 2))):
        own = average[:, color].reshape(slabs * inner, layer, n)
        got = swap(own, near)
        pair = jnp.stack([own, got])
        blocks.append(jnp.stack([pair, swap(pair, far)]))
    blocks = jnp.stack([blocks[0], blocks[1].transpose(1, 0, 2, 3, 4)])
    blocks = jnp.stack([blocks, swap(blocks, 1)])
    for axis, bit in ((0, core), (2, at_y), (3, at_x)):
        blocks = jnp.where(bit == 1, jnp.flip(blocks, axis), blocks)
    return blocks.transpose(5, 0, 1, 2, 3, 4, 6).reshape(layer, n, n), misfits


def solution(mesh):
    placed = (
        P("batch", "slab", None, None),
        P("batch"),
        P("batch"),
        P("batch", None),
        P("slab", None, None),
    )
    return jax.shard_map(
        body, mesh=mesh, in_specs=placed, out_specs=(P("slab", None, None), P()), check_vma=False
    )
```
